256 devices in a mesh: dom: 32 (over y, z), hid: 4 (over x_lo, core), wt: 2 (over x_hi).
Axes of the slice: x: 4 (x_hi: 2, x_lo: 2; x = x_hi * 2 + x_lo), y: 4, z: 8, core: 2. Of those that a mesh axis runs over, the one named last changes fastest.
Arguments:
- store_feat: bfloat16 [131072, 256], P('dom'), may hold values from -6 to 6
- want_in: int32 [32, 32, 128], P('dom'), may hold values from 0 to 4095
- nbr_in: int32 [262144, 10], P('dom'), may hold values from 0 to 4095
- self_in: int32 [262144], P('dom'), may hold values from 0 to 4095
- count_in: int32 [262144], P('dom'), may hold values from 1 to 10
- weight_one: bfloat16 [512, 1024], P('wt', 'hid'), may hold values from -0.375 to 0.375
- want_hid: int32 [32, 32, 128], P('dom'), may hold values from 0 to 8191
- nbr_hid: int32 [65536, 15], P('dom'), may hold values from 0 to 4095
- self_hid: int32 [65536], P('dom'), may hold values from 0 to 4095
- count_hid: int32 [65536], P('dom'), may hold values from 1 to 15
- weight_two: bfloat16 [2048, 1024], P('wt', 'hid'), may hold values from -0.1875 to 0.1875
Outputs:
- seed_embed: bfloat16 [65536, 1024], P('dom', 'hid')
The draws below stay inside these ranges and needn't reach their ends.
Inputs may be any that keep to these rules, and one draw needn't show every extreme that they name: `count_in`: slots at or past a node's count hold arbitrary positions and are ignored. `count_hid`: slots at or past a seed's count hold arbitrary positions and are ignored.
All inputs are finite; a program needn't handle non-finite values.
Results may differ from the reference program's by a relative error of at most 0.0052.
Values may be sent and summed in bfloat16 or wider, within the bound.
No kernel may reach another device: no remote copies, remote signals or barrier semaphores. Data moves between devices by JAX's collectives and lax.ppermute only.
A program may use at most 128 MiB of HBM per device.

```python
import math
import jax
import jax.numpy as jnp
import numpy as np
from jax import lax

F = 256
H = 1024
FAN1 = 10
FAN2 = 15
S_DEV = 4096
R0 = 128
T1 = 8192
R1 = 128
T2 = 2048
NODES = 131072
N_DOM = 32


def touch_ends(result, rng, least, top_value):
    place = [jax.random.randint(jax.random.fold_in(rng, axis), (), 0, length) for axis, length in enumerate(result.shape)]
    main_axis = result.shape.index(max(result.shape))
    next_to = place[:main_axis] + [(place[main_axis] + 1) % result.shape[main_axis]] + place[main_axis + 1:]
    return result.at[tuple(place)].set(least).at[tuple(next_to)].set(top_value)


def block_scale(rng, dims, split, smallest, high):
    def one(position, parts):
        heights = jax.random.uniform(jax.random.fold_in(jax.random.fold_in(rng, 6), position), (parts,), jnp.float32, smallest / len(split), high / len(split))
        return jnp.repeat(jnp.exp(heights), dims[position] // parts).reshape((-1,) + (1,) * (len(dims) - position - 1))

    factor_of = one(*split[0])
    for cut in split[1:]:
        factor_of = factor_of * one(*cut)
    return factor_of


def rank_table(count, skew):
    loads = [(1 << 20) // math.isqrt(standing ** skew) + 1 for standing in range(1, count + 1)]
    scale = 1 + sum(loads) // (1 << 30)
    return np.cumsum(np.array([max(1, weight // scale) for weight in loads]))


def ranked(stream_key, shape, count, lean):
    listing = rank_table(count, lean)
    lot = jax.random.randint(jax.random.fold_in(stream_key, 1), shape, 0, int(listing[count - 1]))
    standing = jnp.searchsorted(jnp.asarray(listing, jnp.int32), lot, side="right")
    return jax.random.permutation(jax.random.fold_in(stream_key, 2), count)[standing].astype(jnp.int32)


def noise(key, extent, scale, limit, split=(), held_as=jnp.bfloat16):
    factor_of = block_scale(key, extent, split, -0.22, 0.18) if split else 1.0
    drawn = jax.random.normal(key, extent, jnp.float32) * scale * factor_of
    return jnp.minimum(jnp.maximum(drawn, -limit), limit).astype(held_as)


def setup_inputs(seed: int = 0) -> dict:
    keys = jax.random.split(jax.random.key(seed), 12)
    return {
        "store_feat": noise(keys[0], (NODES, F), 1.0, 6.0, ((0, 32),)),
        "want_in": touch_ends(jax.random.randint(keys[1], (N_DOM, N_DOM, R0), 0, S_DEV), jax.random.fold_in(keys[1], 1), 0, S_DEV - 1).astype(jnp.int32),
        "nbr_in": touch_ends(ranked(keys[2], (N_DOM * T1, FAN1), N_DOM * R0, 2), jax.random.fold_in(keys[2], 3), 0, (N_DOM * R0) - 1).astype(jnp.int32),
        "self_in": touch_ends(jax.random.randint(keys[3], (N_DOM * T1,), 0, N_DOM * R0), jax.random.fold_in(keys[3], 1), 0, (N_DOM * R0) - 1).astype(jnp.int32),
        "count_in": touch_ends(jax.random.randint(keys[4], (N_DOM * T1,), 1, FAN1 + 1), jax.random.fold_in(keys[4], 1), 1, FAN1).astype(jnp.int32),
        "weight_one": noise(keys[5], (2 * F, H), F ** -0.5, 0.375, ((0, 2), (1, 4))),
        "want_hid": touch_ends(jax.random.randint(keys[6], (N_DOM, N_DOM, R1), 0, T1), jax.random.fold_in(keys[6], 1), 0, T1 - 1).astype(jnp.int32),
        "nbr_hid": touch_ends(ranked(keys[7], (N_DOM * T2, FAN2), N_DOM * R1, 2), jax.random.fold_in(keys[7], 3), 0, (N_DOM * R1) - 1).astype(jnp.int32),
        "self_hid": touch_ends(jax.random.randint(keys[8], (N_DOM * T2,), 0, N_DOM * R1), jax.random.fold_in(keys[8], 1), 0, (N_DOM * R1) - 1).astype(jnp.int32),
        "count_hid": touch_ends(jax.random.randint(keys[9], (N_DOM * T2,), 1, FAN2 + 1), jax.random.fold_in(keys[9], 1), 1, FAN2).astype(jnp.int32),
        "weight_two": noise(keys[10], (2 * H, H), H ** -0.5, 0.1875, ((0, 2), (1, 4))),
    }


def average(lookup, neighbours, counts):
    gathered = jnp.take(lookup, neighbours, axis=0).astype(jnp.float32)
    valid_mask = (lax.broadcasted_iota(jnp.int32, neighbours.shape, 1) < counts[:, None]).astype(jnp.float32)
    summed = jnp.einsum("tk,tkf->tf", valid_mask, gathered)
    return (summed / counts[:, None].astype(jnp.float32)).astype(jnp.bfloat16)


def reference(store_feat, want_in, nbr_in, self_in, count_in, weight_one, want_hid, nbr_hid, self_hid, count_hid, weight_two):
    storage = store_feat.reshape(N_DOM, S_DEV, F)
    owners = jnp.arange(N_DOM, dtype=jnp.int32)[:, None]

    def layer_one(inputs):
        wanted, neighbours, own_pos, counts = inputs
        lookup = storage[owners, wanted].reshape(N_DOM * R0, F)
        own_rows = jnp.take(lookup, own_pos, axis=0)
        mean_rows = average(lookup, neighbours, counts)
        joined = jnp.concatenate([own_rows, mean_rows], 1)
        return jax.nn.relu(jnp.dot(joined, weight_one, preferred_element_type=jnp.float32)).astype(jnp.bfloat16)

    hidden = lax.map(layer_one, (jnp.swapaxes(want_in, 0, 1), nbr_in.reshape(N_DOM, T1, FAN1), self_in.reshape(N_DOM, T1), count_in.reshape(N_DOM, T1)))

    def layer_two(inputs):
        wanted, neighbours, own_pos, counts = inputs
        lookup = hidden[owners, wanted].reshape(N_DOM * R1, H)
        own_rows = jnp.take(lookup, own_pos, axis=0)
        mean_rows = average(lookup, neighbours, counts)
        joined = jnp.concatenate([own_rows, mean_rows], 1)
        return jnp.dot(joined, weight_two, preferred_element_type=jnp.float32).astype(jnp.bfloat16)

    seeds = lax.map(layer_two, (jnp.swapaxes(want_hid, 0, 1), nbr_hid.reshape(N_DOM, T2, FAN2), self_hid.reshape(N_DOM, T2), count_hid.reshape(N_DOM, T2)))
    return seeds.reshape(N_DOM * T2, H)
```

```python
import jax
import jax.numpy as jnp
from jax import lax
from jax.experimental import pallas as pl
from jax.experimental.pallas import tpu as pltpu
from jax.sharding import Mesh, PartitionSpec as P

BF16 = jnp.bfloat16
F32 = jnp.float32
MIB = 1 << 20
CHIPS = 4
LINE = ("xlo", "wt")
SLOTS = 16
LOW = 256


def spot(x):
    return (x % 2) * 2 + x // 2


UP = [(spot(x), spot((x + 1) % CHIPS)) for x in range(CHIPS)]
DOWN = [(spot(x), spot((x - 1) % CHIPS)) for x in range(CHIPS)]
ACROSS = [(spot(x), spot((x + 2) % CHIPS)) for x in range(CHIPS)]
SWAP = [(0, 1), (1, 0)]


def ring_pieces(block):
    half = block.shape[0] // 2
    below = lax.ppermute(block, LINE, UP)
    above = lax.ppermute(block, LINE, DOWN)
    far_low = lax.ppermute(below[:half], LINE, UP)
    far_high = lax.ppermute(above[half:], LINE, DOWN)
    return block, above, far_low, far_high, below


def place(position, x):
    return ((((position >> 5) - x) & 3) << 10) | ((position >> 7) << 5) | (position & 31)


def codes(neighbours, counts, x):
    targets, fan = neighbours.shape
    neighbours = jnp.pad(neighbours, ((0, 0), (0, SLOTS - fan)))
    at = place(neighbours, x)
    valid = lax.broadcasted_iota(jnp.int32, at.shape, 1) < counts[:, None]
    lane = lax.broadcasted_iota(jnp.int32, at.shape, 0) & (SLOTS - 1)
    high = jnp.where(valid, (at >> 8) * SLOTS + lane, -1)
    low = at & (LOW - 1)
    shape = (targets // SLOTS, SLOTS * SLOTS)
    return high.reshape(shape).astype(F32), low.reshape(shape).astype(F32)


def count_kernel(high_ref, low_ref, out_ref):
    groups = high_ref.shape[0]
    rows = lax.broadcasted_iota(jnp.int32, (LOW, LOW), 0).astype(F32).astype(BF16)
    one = jnp.ones((), BF16)
    zero = jnp.zeros((), BF16)
    for g in range(groups):
        high = high_ref[g : g + 1, :].astype(BF16)
        low = low_ref[g : g + 1, :].astype(BF16)
        left = jnp.where(rows == high, one, zero)
        right = jnp.where(rows == low, one, zero)
        counts = lax.dot_general(left, right, (((1,), (1,)), ((), ())), preferred_element_type=F32)
        counts = counts.astype(BF16)
        for k in range(LOW // SLOTS):
            out_ref[g * SLOTS : (g + 1) * SLOTS, k * LOW : (k + 1) * LOW] = counts[
                k * SLOTS : (k + 1) * SLOTS, :
            ]


def count_matrix(high, low, positions):
    groups, width = high.shape
    step = 8
    return pl.pallas_call(
        count_kernel,
        grid=(groups // step,),
        in_specs=[pl.BlockSpec((step, width), lambda i: (i, 0))] * 2,
        out_specs=pl.BlockSpec((step * SLOTS, positions), lambda i: (i, 0)),
        out_shape=jax.ShapeDtypeStruct((groups * SLOTS, positions), BF16),
        compiler_params=pltpu.CompilerParams(vmem_limit_bytes=16 * MIB),
        cost_estimate=pl.CostEstimate(
            flops=groups * 2 * LOW * LOW * LOW,
            transcendentals=0,
            bytes_accessed=groups * SLOTS * positions * 2,
        ),
        name="count_matrix",
    )(high, low)


def one_hot(index, start, width):
    at = lax.broadcasted_iota(jnp.int32, (index.shape[0], width), 1) + start
    return jnp.where(at == index, 1.0, 0.0).astype(BF16)


def dot(a, b):
    return jnp.dot(a, b, preferred_element_type=F32)


def mean_kernel(counts_ref, own_ref, size_ref, *refs):
    pieces, out_ref = refs[:-1], refs[-1]
    width = out_ref.shape[1] // 2
    own_at = own_ref[...]
    own = jnp.zeros((out_ref.shape[0], width), F32)
    total = own
    start = 0
    for piece in pieces:
        rows = piece.shape[0]
        data = piece[...]
        own = own + dot(one_hot(own_at, start, rows), data)
        total = total + dot(counts_ref[:, start : start + rows], data)
        start += rows
    out_ref[:, :width] = own.astype(BF16)
    out_ref[:, width:] = (total / size_ref[...]).astype(BF16)


def own_and_mean(counts, own_at, sizes, pieces):
    targets, positions = counts.shape
    width = pieces[0].shape[1]
    tile = 256
    return pl.pallas_call(
        mean_kernel,
        grid=(targets // tile,),
        in_specs=[
            pl.BlockSpec((tile, positions), lambda i: (i, 0)),
            pl.BlockSpec((tile, 1), lambda i: (i, 0)),
            pl.BlockSpec((tile, 1), lambda i: (i, 0)),
        ]
        + [pl.BlockSpec(p.shape, lambda i: (0, 0)) for p in pieces],
        out_specs=pl.BlockSpec((tile, 2 * width), lambda i: (i, 0)),
        out_shape=jax.ShapeDtypeStruct((targets, 2 * width), BF16),
        compiler_params=pltpu.CompilerParams(vmem_limit_bytes=24 * MIB),
        cost_estimate=pl.CostEstimate(
            flops=4 * targets * positions * width,
            transcendentals=0,
            bytes_accessed=targets * positions * 2,
        ),
        name="own_and_mean",
    )(counts, own_at, sizes, *pieces)


def project_kernel(mine_ref, other_ref, first_ref, second_ref, out_ref):
    k = mine_ref.shape[1]
    acc = dot(mine_ref[...], first_ref[:k, :]) + dot(other_ref[...], first_ref[k:, :])
    hidden = jnp.maximum(acc, 0.0).astype(BF16)
    out_ref[...] = dot(hidden, second_ref[...]).astype(BF16)


def project(mine, other, first, second):
    rows, k = mine.shape
    tile = 256
    width = second.shape[1]
    return pl.pallas_call(
        project_kernel,
        grid=(rows // tile,),
        in_specs=[
            pl.BlockSpec((tile, k), lambda i: (i, 0)),
            pl.BlockSpec((tile, k), lambda i: (i, 0)),
            pl.BlockSpec(first.shape, lambda i: (0, 0)),
            pl.BlockSpec(second.shape, lambda i: (0, 0)),
        ],
        out_specs=pl.BlockSpec((tile, width), lambda i: (i, 0)),
        out_shape=jax.ShapeDtypeStruct((rows, width), BF16),
        compiler_params=pltpu.CompilerParams(vmem_limit_bytes=20 * MIB),
        cost_estimate=pl.CostEstimate(
            flops=2 * rows * first.shape[1] * (2 * k + width),
            transcendentals=0,
            bytes_accessed=rows * (2 * k + width) * 2,
        ),
        name="project",
    )(mine, other, first, second)


def seed_kernel(counts_ref, own_ref, size_ref, *refs):
    pieces, out_ref = refs[:-1], refs[-1]
    width = out_ref.shape[1]
    own_at = own_ref[...]
    own = jnp.zeros((out_ref.shape[0], width), F32)
    total = own
    start = 0
    for piece in pieces:
        rows = piece.shape[0]
        own = own + dot(one_hot(own_at, start, rows), piece[:, :width])
        total = total + dot(counts_ref[:, start : start + rows], piece[:, width:])
        start += rows
    out_ref[...] = (own + total / size_ref[...]).astype(BF16)


def seeds(counts, own_at, sizes, pieces):
    targets, positions = counts.shape
    width = pieces[0].shape[1] // 2
    tile = 256
    return pl.pallas_call(
        seed_kernel,
        grid=(targets // tile,),
        in_specs=[
            pl.BlockSpec((tile, positions), lambda i: (i, 0)),
            pl.BlockSpec((tile, 1), lambda i: (i, 0)),
            pl.BlockSpec((tile, 1), lambda i: (i, 0)),
        ]
        + [pl.BlockSpec(p.shape, lambda i: (0, 0)) for p in pieces],
        out_specs=pl.BlockSpec((tile, width), lambda i: (i, 0)),
        out_shape=jax.ShapeDtypeStruct((targets, width), BF16),
        compiler_params=pltpu.CompilerParams(vmem_limit_bytes=32 * MIB),
        cost_estimate=pl.CostEstimate(
            flops=4 * targets * positions * width,
            transcendentals=0,
            bytes_accessed=targets * positions * 2,
        ),
        name="seeds",
    )(counts, own_at, sizes, *pieces)


def shards(
    store_feat,
    want_in,
    nbr_in,
    self_in,
    count_in,
    weight_one,
    want_hid,
    nbr_hid,
    self_hid,
    count_hid,
    weight_two,
):
    x = lax.axis_index("wt") * 2 + lax.axis_index("xlo")
    core = lax.axis_index("core")
    parts = want_in.shape[1]
    block = want_in.shape[2] // CHIPS
    half = store_feat.shape[1] // 2

    def mine(wanted):
        return lax.dynamic_slice_in_dim(wanted[0], block * x, block, 1).reshape(-1)

    def exchange(rows):
        pieces = rows.reshape(parts, block, rows.shape[1])
        return lax.all_to_all(pieces, "dom", 0, 0, tiled=True).reshape(rows.shape)

    columns = lax.dynamic_slice_in_dim(store_feat, half * core, half, 1)
    picked = columns.at[mine(want_in)].get(mode="promise_in_bounds")
    inputs = ring_pieces(exchange(picked))

    table = jnp.concatenate([nbr_in, self_in[:, None], count_in[:, None]], 1)
    nodes = table.at[mine(want_hid)].get(mode="promise_in_bounds")
    fan = nbr_in.shape[1]
    sizes = nodes[:, fan + 1]
    counts = count_matrix(*codes(nodes[:, :fan], sizes, x), parts * block * CHIPS)
    own_at = place(nodes[:, fan : fan + 1], x)
    ready = own_and_mean(counts, own_at, sizes[:, None].astype(F32), inputs)

    rows = lax.all_to_all(
        jnp.broadcast_to(weight_one[None], (8, *weight_one.shape)), ("xlo", "core", "wt"), 0, 0, tiled=True
    )
    rows = rows.reshape(4, 2, *weight_one.shape)
    first = jnp.moveaxis(rows, 0, 2).reshape(2, 2, half, 4 * weight_one.shape[1])
    first = jnp.swapaxes(first, 0, 1)
    first = jnp.where(core == 0, first, first[::-1]).reshape(4 * half, -1)
    other_rows = lax.ppermute(weight_two, LINE, ACROSS)
    low = lax.axis_index("wt") == 0
    second = jnp.concatenate(
        [jnp.where(low, weight_two, other_rows), jnp.where(low, other_rows, weight_two)], 1
    )

    counts_two = count_matrix(*codes(nbr_hid, count_hid, x), parts * block * CHIPS)
    arrived = ring_pieces(exchange(ready))
    projected = [
        project(piece, lax.ppermute(piece, "core", SWAP), first, second) for piece in arrived
    ]
    return seeds(
        counts_two, place(self_hid, x)[:, None], count_hid[:, None].astype(F32), projected
    )


def solution(mesh):
    mesh = Mesh(mesh.devices.reshape(32, 2, 2, 2), ("dom", "xlo", "core", "wt"))
    columns = ("xlo", "core")
    return jax.shard_map(
        shards,
        mesh=mesh,
        in_specs=(
            P("dom", None),
            P("dom", None, None),
            P("dom", None),
            P("dom"),
            P("dom"),
            P("wt", columns),
            P("dom", None, None),
            P("dom", None),
            P("dom"),
            P("dom"),
            P("wt", columns),
        ),
        out_specs=P("dom", columns),
        check_vma=False,
    )
```

```python
import functools

import jax
import jax.numpy as jnp
from jax import lax
from jax.experimental import pallas as pl
from jax.experimental.pallas import tpu as pltpu
from jax.sharding import Mesh, PartitionSpec as P


BF16 = jnp.bfloat16
F32 = jnp.float32
MIB = 1 << 20
CHIPS = 4
LINE = ("xlo", "wt")
SLOTS = 16
FAN = 10
TOKEN = jax.ShapeDtypeStruct((8, 128), jnp.int32)
LOW = 256


def in_vmem(count):
    return [pl.BlockSpec(memory_space=pltpu.VMEM)] * count


def spot(x):
    return (x % 2) * 2 + x // 2


UP = [(spot(x), spot((x + 1) % CHIPS)) for x in range(CHIPS)]
DOWN = [(spot(x), spot((x - 1) % CHIPS)) for x in range(CHIPS)]
ACROSS = [(spot(x), spot((x + 2) % CHIPS)) for x in range(CHIPS)]
SWAP = [(0, 1), (1, 0)]


def send(block, pairs):
    return lax.ppermute(block, LINE, pairs)


def swap(block):
    return lax.ppermute(block, "core", SWAP)


def place(position, x):
    return ((((position >> 5) - x) & 3) << 10) | ((position >> 7) << 5) | (position & 31)


def write_counts(high, low, out_ref, base):
    slot = lax.broadcasted_iota(jnp.int32, (SLOTS, LOW), 0)
    lane = lax.broadcasted_iota(jnp.int32, (SLOTS, LOW), 1)
    expand = jnp.where((lane & (SLOTS - 1)) == slot, 1.0, 0.0).astype(BF16)
    high = dot(high.astype(F32).astype(BF16), expand)
    low = dot(low.astype(F32).astype(BF16), expand)
    target = lax.broadcasted_iota(jnp.int32, high.shape, 0)
    lane = lax.broadcasted_iota(jnp.int32, high.shape, 1)
    mine = (target & (SLOTS - 1)) == (lane >> 4)
    high = jnp.where(mine, high, -1.0).astype(BF16)
    low = jnp.where(mine, low, 0.0)
    rows = lax.broadcasted_iota(jnp.int32, (LOW, LOW), 0).astype(F32).astype(BF16)
    one = jnp.ones((), BF16)
    zero = jnp.zeros((), BF16)
    for g in range(high.shape[0] // SLOTS):
        mine_high = high[g * SLOTS : (g + 1) * SLOTS, :]
        left = jnp.concatenate(
            [jnp.where(mine_high == jnp.full((), k, BF16), one, zero) for k in range(SLOTS)], 0
        )
        mine_low = jnp.sum(low[g * SLOTS : (g + 1) * SLOTS, :], axis=0, keepdims=True).astype(BF16)
        right = jnp.where(rows == mine_low, one, zero)
        counts = lax.dot_general(left, right, (((1,), (1,)), ((), ())), preferred_element_type=F32)
        counts = counts.astype(BF16)
        store_counts(counts, out_ref, base + g * SLOTS)


def store_counts(counts, out_ref, start):
    start = pl.multiple_of(start, SLOTS)
    for k in range(SLOTS):
        out_ref[pl.ds(start, SLOTS), k * LOW : (k + 1) * LOW] = counts[k * SLOTS : (k + 1) * SLOTS, :]


def table_kernel(slots_ref, own_ref, size_ref, out_ref, lines_ref):
    lines_ref[...] = jnp.zeros(lines_ref.shape, jnp.int32)
    lanes = lines_ref.shape[1]
    width = slots_ref.shape[1]
    base = pl.program_id(0) * width
    for b in range(width // lanes):
        at = slice(b * lanes, (b + 1) * lanes)
        lines_ref[:FAN, :] = slots_ref[:, at]
        lines_ref[FAN : FAN + 1, :] = own_ref[:, at]
        lines_ref[FAN + 1 : FAN + 2, :] = size_ref[:, at]
        start = pl.multiple_of(base + b * lanes, lanes)
        out_ref[pl.ds(start, lanes), :] = lines_ref[...].T


def node_table(slots, own, sizes):
    stored = slots.shape[1]
    step = 1024
    return pl.pallas_call(
        table_kernel,
        grid=(stored // step,),
        in_specs=[pl.BlockSpec((a.shape[0], step), lambda i: (0, i)) for a in (slots, own, sizes)],
        out_specs=in_vmem(1)[0],
        out_shape=jax.ShapeDtypeStruct((stored, SLOTS), jnp.int32),
        scratch_shapes=[pltpu.VMEM((SLOTS, 128), jnp.int32)],
        compiler_params=pltpu.CompilerParams(vmem_limit_bytes=2 * MIB),
        name="node_table",
    )(slots, own, sizes)


def node_kernel(request_ref, x_ref, table_ref, nodes_ref, out_ref, token_ref, rows_ref):
    token_ref[...] = jnp.zeros(token_ref.shape, jnp.int32)
    step = rows_ref.shape[0]
    base = pl.multiple_of(pl.program_id(0) * step, step)
    for i in range(step):
        rows_ref[i : i + 1, :] = table_ref[pl.ds(request_ref[base + i], 1), :]
    rows = rows_ref[...]
    nodes_ref[...] = rows
    size = rows[:, FAN + 1 : FAN + 2]
    at = place(rows, x_ref[0])
    valid = lax.broadcasted_iota(jnp.int32, rows.shape, 1) < size
    high = jnp.where(valid, at >> 8, -1)
    write_counts(high, at & (LOW - 1), out_ref, 0)


def node_counts(requests, x, table, positions):
    targets = requests.shape[0]
    step = 256
    return pl.pallas_call(
        node_kernel,
        grid_spec=pltpu.PrefetchScalarGridSpec(
            num_scalar_prefetch=2,
            grid=(targets // step,),
            in_specs=in_vmem(1),
            out_specs=(
                pl.BlockSpec((step, SLOTS), lambda i, r, x: (i, 0)),
                pl.BlockSpec((step, positions), lambda i, r, x: (i, 0)),
                in_vmem(1)[0],
            ),
            scratch_shapes=[pltpu.VMEM((step, SLOTS), jnp.int32)],
        ),
        out_shape=(
            jax.ShapeDtypeStruct((targets, SLOTS), jnp.int32),
            pltpu.HBM((targets, positions), BF16),
            TOKEN,
        ),
        compiler_params=pltpu.CompilerParams(vmem_limit_bytes=10 * MIB),
        cost_estimate=pl.CostEstimate(
            flops=targets * 2 * SLOTS * LOW * LOW, transcendentals=0, bytes_accessed=targets * positions * 2
        ),
        name="node_counts",
    )(requests, x.reshape(1), table)


def codes(neighbours, counts, x):
    targets, fan = neighbours.shape
    at = place(jnp.pad(neighbours, ((0, 0), (0, SLOTS - fan))), x)
    valid = lax.broadcasted_iota(jnp.int32, at.shape, 1) < counts[:, None]
    target = lax.broadcasted_iota(jnp.int32, at.shape, 0) & (SLOTS - 1)
    high = jnp.where(valid, (at >> 8) * SLOTS + target + 1, 0)
    return (high * LOW + (at & (LOW - 1))).reshape(targets // SLOTS, SLOTS * SLOTS)


def slot_kernel(code_ref, *refs):
    out_ref, token_ref = refs[-2:]
    token_ref[...] = jnp.zeros(token_ref.shape, jnp.int32)
    rows = lax.broadcasted_iota(jnp.int32, (LOW, LOW), 0).astype(F32).astype(BF16)
    one = jnp.ones((), BF16)
    zero = jnp.zeros((), BF16)
    code = code_ref[...]
    high = ((code >> 8) - 1).astype(F32)
    low = (code & (LOW - 1)).astype(F32)
    for g in range(code_ref.shape[0]):
        left = jnp.where(rows == high[g : g + 1, :].astype(BF16), one, zero)
        right = jnp.where(rows == low[g : g + 1, :].astype(BF16), one, zero)
        counts = lax.dot_general(left, right, (((1,), (1,)), ((), ())), preferred_element_type=F32)
        store_counts(counts.astype(BF16), out_ref, g * SLOTS)


def slot_counts(code, positions, part, before=None):
    groups, width = code.shape
    step = 16
    steps = groups // step // 2
    earlier = () if before is None else (before,)
    return pl.pallas_call(
        slot_kernel,
        grid=(steps,),
        in_specs=[pl.BlockSpec((step, width), lambda i: (i + part * steps, 0))]
        + [pl.BlockSpec(memory_space=pl.ANY)] * len(earlier),
        out_specs=(
            pl.BlockSpec((step * SLOTS, positions), lambda i: (i + part * steps, 0)),
            in_vmem(1)[0],
        ),
        out_shape=(pltpu.HBM((groups * SLOTS, positions), BF16), TOKEN),
        input_output_aliases={1: 0} if earlier else {},
        compiler_params=pltpu.CompilerParams(vmem_limit_bytes=10 * MIB),
        cost_estimate=pl.CostEstimate(
            flops=groups * LOW * LOW * LOW,
            transcendentals=0,
            bytes_accessed=groups // 2 * SLOTS * positions * 2,
        ),
        name="slot_counts",
    )(code, *earlier)


def weight_kernel(at_ref, *refs):
    blocks, (mine_ref, other_ref, first_ref, second_ref, token_ref) = refs[:-5], refs[-5:]
    token_ref[...] = jnp.zeros(token_ref.shape, jnp.int32)
    x, core = at_ref[0], at_ref[1]
    half = first_ref.shape[1] // 4
    for i, block in enumerate(blocks):
        chip = (x + i // 2) & (CHIPS - 1)
        column = 2 * (chip & 1) + (core if i % 2 == 0 else 1 - core)
        for side in range(2):
            start = pl.multiple_of(half * (core if side == 0 else 1 - core), half)
            at = pl.multiple_of((2 * side + (chip >> 1)) * half, half)
            first_ref[column, pl.ds(at, half), :] = block[pl.ds(start, half), :]
    columns = mine_ref.shape[1]

    @pl.when(x < 2)
    def _():
        second_ref[:, :columns] = mine_ref[...]
        second_ref[:, columns:] = other_ref[...]

    @pl.when(x >= 2)
    def _():
        second_ref[:, :columns] = other_ref[...]
        second_ref[:, columns:] = mine_ref[...]


def assemble(at, blocks, mine, other):
    k, width = blocks[0].shape
    first = (CHIPS, 2 * k, width)
    second = (mine.shape[0], 2 * mine.shape[1])
    return pl.pallas_call(
        weight_kernel,
        grid_spec=pltpu.PrefetchScalarGridSpec(
            num_scalar_prefetch=1,
            grid=(1,),
            in_specs=[
                pl.BlockSpec(b.shape, lambda i, at: (0, 0), pipeline_mode=pl.Buffered(1))
                for b in (*blocks, mine, other)
            ],
            out_specs=tuple(in_vmem(3)),
        ),
        out_shape=(jax.ShapeDtypeStruct(first, BF16), jax.ShapeDtypeStruct(second, BF16), TOKEN),
        compiler_params=pltpu.CompilerParams(vmem_limit_bytes=10 * MIB),
        name="assemble",
    )(at, *blocks, mine, other)


def column(row):
    shape = (row.shape[1], row.shape[1])
    diagonal = lax.broadcasted_iota(jnp.int32, shape, 0) == lax.broadcasted_iota(jnp.int32, shape, 1)
    return jnp.sum(jnp.where(diagonal, row.astype(F32), 0.0), axis=1, keepdims=True)


def dot(a, b):
    return jnp.dot(a, b, preferred_element_type=F32)


def load_rows(out_ref, data_ref, positions):
    for i, at in enumerate(positions):
        out_ref[i : i + 1, :] = data_ref[pl.ds(at, 1), :]


def mean_kernel(tokens, request_ref, place_ref, counts_ref, nodes_ref, *refs):
    pieces, (out_ref, data_ref, wide_ref, own_ref) = refs[tokens:-4], refs[-4:]
    tile, width = out_ref.shape[0], out_ref.shape[1] // 2

    @pl.when(pl.program_id(0) == 0)
    def _():
        start = 0
        for piece in pieces:
            data = piece[...]
            data_ref[start : start + piece.shape[0], :] = data
            wide_ref[start : start + piece.shape[0], :] = data.astype(F32)
            start += piece.shape[0]

    base = pl.program_id(0) * tile
    load_rows(own_ref, wide_ref, [place_ref[request_ref[base + i]] for i in range(tile)])
    size = nodes_ref[:, FAN + 1 : FAN + 2].astype(F32)
    total = dot(counts_ref[...], data_ref[...])
    out_ref[:, width:] = (total / size).astype(BF16)
    out_ref[:, :width] = own_ref[...].astype(BF16)


def own_and_mean(requests, places, counts, nodes, pieces, after):
    targets, positions = counts.shape
    width = pieces[0].shape[1]
    tile = 256
    return pl.pallas_call(
        functools.partial(mean_kernel, len(after)),
        grid_spec=pltpu.PrefetchScalarGridSpec(
            num_scalar_prefetch=2,
            grid=(targets // tile,),
            in_specs=[
                pl.BlockSpec((tile, positions), lambda i, r, p: (i, 0)),
                pl.BlockSpec((tile, SLOTS), lambda i, r, p: (i, 0)),
            ]
            + in_vmem(len(after) + len(pieces)),
            out_specs=pl.BlockSpec((tile, 2 * width), lambda i, r, p: (i, 0)),
            scratch_shapes=[
                pltpu.VMEM((positions, width), BF16),
                pltpu.VMEM((positions, width), F32),
                pltpu.VMEM((tile, width), F32),
            ],
        ),
        out_shape=pltpu.HBM((targets, 2 * width), BF16),
        compiler_params=pltpu.CompilerParams(vmem_limit_bytes=14 * MIB),
        cost_estimate=pl.CostEstimate(
            flops=4 * targets * positions * width,
            transcendentals=0,
            bytes_accessed=targets * positions * 2,
        ),
        name="own_and_mean",
    )(requests, places, pltpu.with_memory_space_constraint(counts, pltpu.HBM), nodes, *after, *pieces)


def project_into(self_ref, near_ref, start, mine_ref, other_ref, first_ref, second_ref):
    rows, k = mine_ref.shape
    tile = min(rows, 512)
    columns = self_ref.shape[1]
    for at in range(0, rows, tile):
        mine, other = mine_ref[at : at + tile, :], other_ref[at : at + tile, :]
        acc = jnp.zeros((tile, 2 * columns), F32)
        for h in range(first_ref.shape[0]):
            pre = dot(mine, first_ref[h, :k, :]) + dot(other, first_ref[h, k:, :])
            hidden = jnp.maximum(pre, 0.0).astype(BF16)
            width = hidden.shape[1]
            acc = acc + dot(hidden, second_ref[h * width : (h + 1) * width, :])
        self_ref[start + at : start + at + tile, :] = acc[:, :columns]
        near_ref[start + at : start + at + tile, :] = acc[:, columns:].astype(BF16)


def project_kernel(tokens, first_ref, second_ref, *refs):
    pieces, outs = refs[tokens:-2], refs[-2:]
    start = 0
    for mine, other in zip(pieces[::2], pieces[1::2]):
        project_into(*outs, start, mine, other, first_ref, second_ref)
        start += mine.shape[0]


def project(first, second, *pieces, after=()):
    rows = sum(p.shape[0] for p in pieces[::2])
    k, width = pieces[0].shape[1], second.shape[1] // 2
    return pl.pallas_call(
        functools.partial(project_kernel, len(after)),
        in_specs=in_vmem(2 + len(after) + len(pieces)),
        out_specs=tuple(in_vmem(2)),
        out_shape=(jax.ShapeDtypeStruct((rows, width), F32), jax.ShapeDtypeStruct((rows, width), BF16)),
        compiler_params=pltpu.CompilerParams(vmem_limit_bytes=8 * MIB),
        cost_estimate=pl.CostEstimate(
            flops=4 * rows * second.shape[0] * (k + width),
            transcendentals=0,
            bytes_accessed=rows * (2 * k + 3 * width) * 2,
        ),
        name="project",
    )(first, second, *after, *pieces)


def seed_kernel(place_ref, counts_ref, size_ref, first_ref, second_ref, *refs):
    pieces, far, (out_ref, self_ref, near_ref, own_ref) = refs[:4], refs[4:-4], refs[-4:]
    tile = out_ref.shape[0]
    block = pieces[0].shape[0]

    @pl.when(pl.program_id(0) == 0)
    def _():
        for out, (own, near) in ((self_ref, pieces[::2]), (near_ref, pieces[1::2])):
            out[:block, :] = own[...]
            out[block : 2 * block, :] = near[:block, :]
            out[3 * block :, :] = near[block:, :]
        start = 2 * block
        for mine, other in zip(far[::2], far[1::2]):
            project_into(self_ref, near_ref, start, mine, other, first_ref, second_ref)
            start += mine.shape[0]

    base = pl.program_id(0) * tile
    load_rows(own_ref, self_ref, [place_ref[base + i] for i in range(tile)])
    total = dot(counts_ref[...], near_ref[...])
    out_ref[...] = (own_ref[...] + total / column(size_ref[...])).astype(BF16)


def seeds(places, counts, sizes, first, second, own, near, far):
    targets, positions = counts.shape
    width = second.shape[1] // 2
    tile = 256
    return pl.pallas_call(
        seed_kernel,
        grid_spec=pltpu.PrefetchScalarGridSpec(
            num_scalar_prefetch=1,
            grid=(targets // tile,),
            in_specs=[
                pl.BlockSpec((tile, positions), lambda i, p: (i, 0)),
                pl.BlockSpec((1, tile), lambda i, p: (0, i)),
            ]
            + in_vmem(6 + len(far)),
            out_specs=pl.BlockSpec((tile, width), lambda i, p: (i, 0)),
            scratch_shapes=[
                pltpu.VMEM((positions, width), F32),
                pltpu.VMEM((positions, width), BF16),
                pltpu.VMEM((tile, width), F32),
            ],
        ),
        out_shape=jax.ShapeDtypeStruct((targets, width), BF16),
        compiler_params=pltpu.CompilerParams(vmem_limit_bytes=18 * MIB),
        cost_estimate=pl.CostEstimate(
            flops=2 * targets * positions * width,
            transcendentals=0,
            bytes_accessed=targets * positions * 2,
        ),
        name="seeds",
    )(places, pltpu.with_memory_space_constraint(counts, pltpu.HBM), sizes, first, second, *own, *near, *far)


def shards(
    store_feat,
    want_in,
    nbr_in,
    self_in,
    count_in,
    weight_one,
    want_hid,
    nbr_hid,
    self_hid,
    count_hid,
    weight_two,
):
    x = lax.axis_index("wt") * 2 + lax.axis_index("xlo")
    core = lax.axis_index("core")
    parts = want_in.shape[1]
    block = want_in.shape[2] // CHIPS
    half = store_feat.shape[1] // 2

    def mine(wanted):
        return lax.dynamic_slice_in_dim(wanted[0], block * x, block, 1).reshape(-1)

    def exchange(rows):
        pieces = rows.reshape(parts, block, rows.shape[1])
        return lax.all_to_all(pieces, "dom", 0, 0, tiled=True).reshape(rows.shape)

    together = lax.optimization_barrier
    positions = parts * block * CHIPS

    picked = store_feat.at[mine(want_in)].get(mode="promise_in_bounds")
    picked = lax.dynamic_slice_in_dim(picked, half * core, half, 1)
    fetched = exchange(picked)

    table = node_table(nbr_in.T, self_in[None], count_in[None])
    requests = mine(want_hid)
    nodes, counts, token = node_counts(requests, x, table, positions)
    fetched, token = together((fetched, token))
    below, above = send(fetched, UP), send(fetched, DOWN)
    code = codes(nbr_hid, count_hid, x)
    places = place(self_in, x)
    below, above, code, places = together((below, above, code, places))
    cut = below.shape[0] // 2
    far_low, far_high = send(below[:cut], UP), send(above[cut:], DOWN)
    counts_two, token_two = slot_counts(code, positions, 0)
    weight_one, token_two = together((weight_one, token_two))
    first_blocks = [weight_one] + [send(weight_one, pairs) for pairs in (DOWN, ACROSS, UP)]
    pieces = (fetched, above, far_low, far_high, below)
    ready = own_and_mean(requests, places, counts, nodes, pieces, (token, token_two))

    ready, weight_two, code, *first_blocks = together((ready, weight_two, code, *first_blocks))
    arrived = exchange(ready)
    other_rows = send(weight_two, ACROSS)
    counts_two, token = slot_counts(code, positions, 1, counts_two)
    first_blocks = [b for block in first_blocks for b in (block, swap(block))]
    own_at = place(self_hid, x)
    arrived, own_at, token, weight_two, other_rows, *first_blocks = together(
        (arrived, own_at, token, weight_two, other_rows, *first_blocks)
    )
    at = jnp.stack([x, core]).astype(jnp.int32)
    first, second, ready = assemble(at, first_blocks, weight_two, other_rows)
    cut = arrived.shape[0] // 2
    low, high = arrived[:cut], arrived[cut:]
    below_low, above_high = send(low, UP), send(high, DOWN)
    below_high, above_low = send(high, UP), send(low, DOWN)
    other = swap(arrived)
    below_low, above_high, other, ready = together((below_low, above_high, other, ready))
    far_low = send(below_low, UP)
    far_high = send(above_high, DOWN)
    own = project(first, second, arrived, other, after=(token, ready))
    below_high, above_low, *own = together((below_high, above_low, *own))
    near = []
    for piece in (above_low, above_high, below_low, below_high):
        near += [piece, swap(piece)]
    near = project(first, second, *near)
    far_low, far_high, *near = together((far_low, far_high, *near))
    far = (far_low, swap(far_low), far_high, swap(far_high))
    return seeds(own_at, counts_two, count_hid[None], first, second, own, near, far)


def solution(mesh):
    mesh = Mesh(mesh.devices.reshape(32, 2, 2, 2), ("dom", "xlo", "core", "wt"))
    columns = ("xlo", "core")
    return jax.shard_map(
        shards,
        mesh=mesh,
        in_specs=(
            P("dom", None),
            P("dom", None, None),
            P("dom", None),
            P("dom"),
            P("dom"),
            P("wt", columns),
            P("dom", None, None),
            P("dom", None),
            P("dom"),
            P("dom"),
            P("wt", columns),
        ),
        out_specs=P("dom", columns),
        check_vma=False,
    )
```

```python
import functools

import jax
import jax.numpy as jnp
from jax import lax
from jax.experimental import pallas as pl
from jax.experimental.pallas import tpu as pltpu
from jax.sharding import Mesh, PartitionSpec as P


BF16 = jnp.bfloat16
F32 = jnp.float32
MIB = 1 << 20
CHIPS = 4
LINE = ("xlo", "wt")
SLOTS = 16
FAN = 10
TOKEN = pltpu.HBM((8, 128), jnp.int32)
SPLIT = 4
LOW = 256


def in_place(count):
    return [pl.BlockSpec(memory_space=pl.ANY)] * count


def to_hbm(array):
    return pltpu.with_memory_space_constraint(array, pltpu.HBM)


def in_vmem(count):
    return [pl.BlockSpec(memory_space=pltpu.VMEM)] * count


def spot(x):
    return (x % 2) * 2 + x // 2


UP = [(spot(x), spot((x + 1) % CHIPS)) for x in range(CHIPS)]
DOWN = [(spot(x), spot((x - 1) % CHIPS)) for x in range(CHIPS)]
ACROSS = [(spot(x), spot((x + 2) % CHIPS)) for x in range(CHIPS)]
SWAP = [(0, 1), (1, 0)]


def send(block, pairs):
    return lax.ppermute(block, LINE, pairs)


def swap(block):
    return lax.ppermute(block, "core", SWAP)


def place(position, x):
    return ((((position >> 5) - x) & 3) << 10) | ((position >> 7) << 5) | (position & 31)


def write_counts(high, low, out_refs):
    slot = lax.broadcasted_iota(jnp.int32, (SLOTS, LOW), 0)
    lane = lax.broadcasted_iota(jnp.int32, (SLOTS, LOW), 1)
    expand = jnp.where((lane & (SLOTS - 1)) == slot, 1.0, 0.0).astype(BF16)
    high = dot(high.astype(F32).astype(BF16), expand)
    low = dot(low.astype(F32).astype(BF16), expand)
    target = lax.broadcasted_iota(jnp.int32, high.shape, 0)
    lane = lax.broadcasted_iota(jnp.int32, high.shape, 1)
    mine = (target & (SLOTS - 1)) == (lane >> 4)
    high = jnp.where(mine, high, -1.0).astype(BF16)
    low = jnp.where(mine, low, 0.0)
    rows = lax.broadcasted_iota(jnp.int32, (LOW, LOW), 0).astype(F32).astype(BF16)
    one = jnp.ones((), BF16)
    zero = jnp.zeros((), BF16)
    for g in range(high.shape[0] // SLOTS):
        mine_high = high[g * SLOTS : (g + 1) * SLOTS, :]
        left = jnp.concatenate(
            [jnp.where(mine_high == jnp.full((), k, BF16), one, zero) for k in range(SLOTS)], 0
        )
        mine_low = jnp.sum(low[g * SLOTS : (g + 1) * SLOTS, :], axis=0, keepdims=True).astype(BF16)
        right = jnp.where(rows == mine_low, one, zero)
        counts = lax.dot_general(left, right, (((1,), (1,)), ((), ())), preferred_element_type=F32)
        counts = counts.astype(BF16)
        store_counts(counts, out_refs, g * SLOTS)


def store_counts(counts, out_refs, start):
    each = SLOTS // SPLIT
    for k in range(SLOTS):
        out_refs[k // each][pl.ds(start, SLOTS), k % each * LOW : (k % each + 1) * LOW] = counts[
            k * SLOTS : (k + 1) * SLOTS, :
        ]


def rows_at(index, data_ref):
    rows = index.shape[0]
    lane = lax.broadcasted_iota(jnp.int32, (rows, LOW), 1).astype(F32).astype(BF16)
    spread = lambda a: jnp.broadcast_to(a.astype(F32), (rows, LOW)).astype(BF16)
    found = jnp.where(lane == spread(index & (LOW - 1)), spread(index >> 8), jnp.full((), -1, BF16))
    one, zero = jnp.ones((), BF16), jnp.zeros((), BF16)
    step = data_ref.shape[0] // SPLIT
    total = 0.0
    for start in range(0, data_ref.shape[0], step):
        hot = [
            jnp.where(found == jnp.full((), k, BF16), one, zero)
            for k in range(start // LOW, (start + step) // LOW)
        ]
        total = total + dot(jnp.concatenate(hot, 1), data_ref[start : start + step, :])
    return total


def counted(copy, buffer_ref, first, data_ref):
    step = data_ref.shape[0] // SPLIT
    total = 0.0
    for k in range(SPLIT):
        copy(first + k).wait()
        total = total + dot(buffer_ref[first + k], data_ref[k * step : (k + 1) * step, :])
    return total


def fetch_counts(counts_refs, buffer_ref, sems):
    rows = buffer_ref.shape[1]
    for k in range(buffer_ref.shape[0]):
        part = k // SPLIT * rows
        source = counts_refs[k % SPLIT].at[part : part + rows, :]
        pltpu.make_async_copy(source, buffer_ref.at[k], sems.at[k]).start()
    source = counts_refs[0].at[:rows, :]
    return lambda k: pltpu.make_async_copy(source, buffer_ref.at[k], sems.at[k])


def table_kernel(slots_ref, own_ref, size_ref, out_ref, lines_ref):
    lines_ref[...] = jnp.zeros(lines_ref.shape, jnp.int32)
    lanes = lines_ref.shape[1]
    width = slots_ref.shape[1]
    base = pl.program_id(0) * width
    for b in range(width // lanes):
        at = slice(b * lanes, (b + 1) * lanes)
        lines_ref[:FAN, :] = slots_ref[:, at]
        lines_ref[FAN : FAN + 1, :] = own_ref[:, at]
        lines_ref[FAN + 1 : FAN + 2, :] = size_ref[:, at]
        start = pl.multiple_of(base + b * lanes, lanes)
        out_ref[pl.ds(start, lanes), :] = lines_ref[...].T


def node_table(slots, own, sizes):
    stored = slots.shape[1]
    step = 512
    return pl.pallas_call(
        table_kernel,
        grid=(stored // step,),
        in_specs=[pl.BlockSpec((a.shape[0], step), lambda i: (0, i)) for a in (slots, own, sizes)],
        out_specs=in_vmem(1)[0],
        out_shape=jax.ShapeDtypeStruct((stored, SLOTS), jnp.int32),
        scratch_shapes=[pltpu.VMEM((SLOTS, 128), jnp.int32)],
        compiler_params=pltpu.CompilerParams(vmem_limit_bytes=2 * MIB),
        name="node_table",
    )(slots, own, sizes)


def node_kernel(request_ref, x_ref, table_ref, nodes_ref, *refs):
    out_refs, rows_ref = refs[:SPLIT], refs[-1]
    step = rows_ref.shape[0]
    base = pl.multiple_of(pl.program_id(0) * step, step)

    @pl.loop(0, step, step=32)
    def _(start):
        for i in range(32):
            rows_ref[pl.ds(start + i, 1), :] = table_ref[pl.ds(request_ref[base + start + i], 1), :]

    rows = rows_ref[...]
    nodes_ref[...] = rows
    size = rows[:, FAN + 1 : FAN + 2]
    at = place(rows, x_ref[0])
    valid = lax.broadcasted_iota(jnp.int32, rows.shape, 1) < size
    high = jnp.where(valid, at >> 8, -1)
    write_counts(high, at & (LOW - 1), out_refs)


def node_counts(requests, x, table, positions):
    targets = requests.shape[0]
    step = 128
    return pl.pallas_call(
        node_kernel,
        grid_spec=pltpu.PrefetchScalarGridSpec(
            num_scalar_prefetch=2,
            grid=(targets // step,),
            in_specs=in_vmem(1),
            out_specs=(
                *[pl.BlockSpec((step, SLOTS), lambda i, r, x: (i, 0))],
                *[pl.BlockSpec((step, positions // SPLIT), lambda i, r, x: (i, 0))] * SPLIT,
                *in_place(1),
            ),
            scratch_shapes=[pltpu.VMEM((step, SLOTS), jnp.int32)],
        ),
        out_shape=(
            pltpu.HBM((targets, SLOTS), jnp.int32),
            *[pltpu.HBM((targets, positions // SPLIT), BF16)] * SPLIT,
            TOKEN,
        ),
        compiler_params=pltpu.CompilerParams(vmem_limit_bytes=10 * MIB),
        cost_estimate=pl.CostEstimate(
            flops=targets * 2 * SLOTS * LOW * LOW, transcendentals=0, bytes_accessed=targets * positions * 2
        ),
        name="node_counts",
    )(requests, x.reshape(1), table)


def codes(neighbours, counts, x):
    targets, fan = neighbours.shape
    at = place(jnp.pad(neighbours, ((0, 0), (0, SLOTS - fan))), x)
    valid = lax.broadcasted_iota(jnp.int32, at.shape, 1) < counts[:, None]
    target = lax.broadcasted_iota(jnp.int32, at.shape, 0) & (SLOTS - 1)
    high = jnp.where(valid, (at >> 8) * SLOTS + target + 1, 0)
    return (high * LOW + (at & (LOW - 1))).reshape(targets // SLOTS, SLOTS * SLOTS)


def slot_kernel(code_ref, *refs):
    out_refs = refs[-SPLIT - 1 : -1]
    rows = lax.broadcasted_iota(jnp.int32, (LOW, LOW), 0).astype(F32).astype(BF16)
    one = jnp.ones((), BF16)
    zero = jnp.zeros((), BF16)

    @pl.loop(0, code_ref.shape[0], step=4)
    def _(first):
        for i in range(4):
            code = code_ref[pl.ds(first + i, 1), :]
            left = jnp.where(rows == ((code >> 8) - 1).astype(F32).astype(BF16), one, zero)
            right = jnp.where(rows == (code & (LOW - 1)).astype(F32).astype(BF16), one, zero)
            counts = lax.dot_general(left, right, (((1,), (1,)), ((), ())), preferred_element_type=F32)
            store_counts(counts.astype(BF16), out_refs, pl.multiple_of((first + i) * SLOTS, SLOTS))


def slot_counts(code, positions, part, before=()):
    groups, width = code.shape
    step = 8
    steps = groups // step // 2
    width_out = positions // SPLIT
    return pl.pallas_call(
        slot_kernel,
        grid=(steps,),
        in_specs=[pl.BlockSpec((step, width), lambda i: (i + part * steps, 0))]
        + in_place(len(before)),
        out_specs=(
            *[pl.BlockSpec((step * SLOTS, width_out), lambda i: (i + part * steps, 0))] * SPLIT,
            *in_place(1),
        ),
        out_shape=(*[pltpu.HBM((groups * SLOTS, width_out), BF16)] * SPLIT, TOKEN),
        input_output_aliases={i + 1: i for i in range(len(before))},
        compiler_params=pltpu.CompilerParams(vmem_limit_bytes=10 * MIB),
        cost_estimate=pl.CostEstimate(
            flops=groups * LOW * LOW * LOW,
            transcendentals=0,
            bytes_accessed=groups // 2 * SLOTS * positions * 2,
        ),
        name="slot_counts",
    )(code, *before)


def weight_kernel(at_ref, *refs):
    blocks, (mine_ref, other_ref, first_ref, second_ref, token_ref) = refs[:-5], refs[-5:]
    x, core = at_ref[0], at_ref[1]
    half = first_ref.shape[1] // 4
    for i, block in enumerate(blocks):
        chip = (x + i // 2) & (CHIPS - 1)
        column = 2 * (chip & 1) + (core if i % 2 == 0 else 1 - core)
        for side in range(2):
            start = pl.multiple_of(half * (core if side == 0 else 1 - core), half)
            at = pl.multiple_of((2 * side + (chip >> 1)) * half, half)
            first_ref[column, pl.ds(at, half), :] = block[pl.ds(start, half), :]
    columns = mine_ref.shape[1]

    def join(left_ref, right_ref):
        @pl.loop(0, second_ref.shape[0] // half)
        def _(i):
            rows = pl.ds(pl.multiple_of(i * half, half), half)
            second_ref[rows, :columns] = left_ref[rows, :]
            second_ref[rows, columns:] = right_ref[rows, :]

    pl.when(x < 2)(lambda: join(mine_ref, other_ref))
    pl.when(x >= 2)(lambda: join(other_ref, mine_ref))


def assemble(at, blocks, mine, other):
    k, width = blocks[0].shape
    first = (CHIPS, 2 * k, width)
    second = (mine.shape[0], 2 * mine.shape[1])
    return pl.pallas_call(
        weight_kernel,
        grid_spec=pltpu.PrefetchScalarGridSpec(
            num_scalar_prefetch=1,
            grid=(1,),
            in_specs=[
                pl.BlockSpec(b.shape, lambda i, at: (0, 0), pipeline_mode=pl.Buffered(1))
                for b in (*blocks, mine, other)
            ],
            out_specs=(*in_vmem(2), *in_place(1)),
        ),
        out_shape=(jax.ShapeDtypeStruct(first, BF16), jax.ShapeDtypeStruct(second, BF16), TOKEN),
        compiler_params=pltpu.CompilerParams(vmem_limit_bytes=10 * MIB),
        name="assemble",
    )(at, *[to_hbm(b) for b in (*blocks, mine, other)])


def column(row):
    shape = (row.shape[1], row.shape[1])
    diagonal = lax.broadcasted_iota(jnp.int32, shape, 0) == lax.broadcasted_iota(jnp.int32, shape, 1)
    return jnp.sum(jnp.where(diagonal, row.astype(F32), 0.0), axis=1, keepdims=True)


def dot(a, b):
    return jnp.dot(a, b, preferred_element_type=F32)


def load_rows(out_ref, data_ref, positions):
    for i, at in enumerate(positions):
        out_ref[i : i + 1, :] = data_ref[pl.ds(at, 1), :]


def pick_kernel(want_ref, at_ref, *refs):
    blocks, (out_ref, wide_ref, rows_ref) = refs[:-3], refs[-3:]
    start = 0
    for block in blocks:
        wide_ref[start : start + block.shape[0], :] = block[...].astype(F32)
        start += block.shape[0]
    parts = want_ref.shape[0]
    block = out_ref.shape[0] // parts
    base = at_ref[0] * block

    @pl.loop(0, parts)
    def _(p):
        load_rows(rows_ref, wide_ref, [want_ref[p, base + i] for i in range(block)])
        out_ref[pl.ds(pl.multiple_of(p * block, block), block), :] = rows_ref[...].astype(BF16)


def pick(want, at, stored, targets):
    rows, width = stored.shape[0] // SPLIT, stored.shape[1] // 2
    block = targets // want.shape[0]
    return pl.pallas_call(
        pick_kernel,
        grid_spec=pltpu.PrefetchScalarGridSpec(
            num_scalar_prefetch=2,
            grid=(1,),
            in_specs=[
                pl.BlockSpec((rows, width), lambda i, w, at, k=k: (k, at[1])) for k in range(SPLIT)
            ],
            out_specs=pl.BlockSpec((targets, width), lambda i, w, at: (0, 0)),
            scratch_shapes=[
                pltpu.VMEM((stored.shape[0], width), F32),
                pltpu.VMEM((block, width), F32),
            ],
        ),
        out_shape=jax.ShapeDtypeStruct((targets, width), BF16),
        compiler_params=pltpu.CompilerParams(vmem_limit_bytes=8 * MIB),
        name="pick",
    )(want, at, *[to_hbm(stored)] * SPLIT)


def mean_kernel(tokens, x_ref, *refs):
    counts_refs, nodes_ref, refs = refs[:SPLIT], refs[SPLIT], refs[SPLIT + 1 :]
    pieces, (out_ref, data_ref, buffer_ref, sems) = refs[tokens:-4], refs[-4:]
    width = out_ref.shape[1] // 2
    copy = fetch_counts(counts_refs, buffer_ref, sems)
    start = 0
    for piece in pieces:
        data_ref[start : start + piece.shape[0], :] = piece[...]
        start += piece.shape[0]
    own_at = place(nodes_ref[:, FAN : FAN + 1], x_ref[0])
    size = nodes_ref[:, FAN + 1 : FAN + 2].astype(F32)
    out_ref[:, :width] = rows_at(own_at, data_ref).astype(BF16)
    total = counted(copy, buffer_ref, 0, data_ref)
    out_ref[:, width:] = (total / size).astype(BF16)


def own_and_mean(x, counts, nodes, pieces, after):
    targets, each = counts[0].shape
    width = pieces[0].shape[1]
    return pl.pallas_call(
        functools.partial(mean_kernel, len(after)),
        grid_spec=pltpu.PrefetchScalarGridSpec(
            num_scalar_prefetch=1,
            grid=(1,),
            in_specs=in_place(SPLIT)
            + [pl.BlockSpec(nodes.shape, lambda i, x: (0, 0))]
            + in_place(len(after))
            + in_vmem(len(pieces)),
            out_specs=pl.BlockSpec((targets, 2 * width), lambda i, x: (0, 0)),
            scratch_shapes=[
                pltpu.VMEM((SPLIT * each, width), BF16),
                pltpu.VMEM((SPLIT, targets, each), BF16),
                pltpu.SemaphoreType.DMA((SPLIT,)),
            ],
        ),
        out_shape=pltpu.HBM((targets, 2 * width), BF16),
        compiler_params=pltpu.CompilerParams(vmem_limit_bytes=24 * MIB),
        cost_estimate=pl.CostEstimate(
            flops=4 * targets * SPLIT * each * width,
            transcendentals=0,
            bytes_accessed=targets * SPLIT * each * 2,
        ),
        name="own_and_mean",
    )(x.reshape(1), *[to_hbm(c) for c in counts], to_hbm(nodes), *map(to_hbm, after), *pieces)


def project_into(out_ref, start, sides, first_ref, second_ref):
    mine, other = (side[...] for side in sides)
    rows, k = mine.shape
    acc = jnp.zeros((rows, out_ref.shape[1]), F32)
    for h in range(first_ref.shape[0]):
        pre = dot(mine, first_ref[h, :k, :]) + dot(other, first_ref[h, k:, :])
        hidden = jnp.maximum(pre, 0.0).astype(BF16)
        width = hidden.shape[1]
        acc = acc + dot(hidden, second_ref[h * width : (h + 1) * width, :])
    out_ref[pl.ds(start, rows), :] = acc.astype(BF16)


def stage(side_refs, pieces):
    start = 0
    for mine, other in zip(pieces[::2], pieces[1::2]):
        for side, piece in zip(side_refs, (mine, other)):
            side[start : start + piece.shape[0], :] = piece[...]
        start += mine.shape[0]


def project_kernel(tokens, first_ref, second_ref, *refs):
    pieces, (out_ref, mine_ref, other_ref) = refs[tokens:-3], refs[-3:]
    if len(pieces) == 2:
        project_into(out_ref, 0, pieces, first_ref, second_ref)
        return
    stage((mine_ref, other_ref), pieces)
    rows = 1024

    @pl.loop(0, out_ref.shape[0] // rows)
    def _(part):
        at = pl.multiple_of(part * rows, rows)
        sides = [side.at[pl.ds(at, rows), :] for side in (mine_ref, other_ref)]
        project_into(out_ref, at, sides, first_ref, second_ref)


def project(first, second, *pieces, after=()):
    rows = sum(p.shape[0] for p in pieces[::2])
    k, width = pieces[0].shape[1], second.shape[1]
    return pl.pallas_call(
        functools.partial(project_kernel, len(after)),
        in_specs=in_vmem(2) + in_place(len(after)) + in_vmem(len(pieces)),
        out_specs=in_vmem(1)[0],
        out_shape=jax.ShapeDtypeStruct((rows, width), BF16),
        scratch_shapes=[pltpu.VMEM((rows, k), BF16)] * 2,
        compiler_params=pltpu.CompilerParams(vmem_limit_bytes=10 * MIB),
        cost_estimate=pl.CostEstimate(
            flops=2 * rows * second.shape[0] * (2 * k + width),
            transcendentals=0,
            bytes_accessed=rows * (2 * k + width) * 2,
        ),
        name="project",
    )(first, second, *map(to_hbm, after), *pieces)


def seed_kernel(*refs):
    counts_refs, (own_ref, size_ref, first_ref, second_ref), refs = refs[:SPLIT], refs[SPLIT : SPLIT + 4], refs[SPLIT + 4 :]
    (mine_ref, near_ref), far, refs = refs[:2], refs[2:-6], refs[-6:]
    out_ref, data_ref, buffer_ref, sides, sems = *refs[:3], refs[3:5], refs[5]
    width = out_ref.shape[1]
    block = mine_ref.shape[0]
    copy = fetch_counts(counts_refs, buffer_ref, sems)
    data_ref[:block, :] = mine_ref[...]
    data_ref[block : 2 * block, :] = near_ref[:block, :]
    data_ref[3 * block :, :] = near_ref[block:, :]
    stage(sides, far)
    project_into(data_ref, 2 * block, sides, first_ref, second_ref)
    rows = buffer_ref.shape[1]

    @pl.loop(0, out_ref.shape[0] // rows)
    def _(part):
        places, sizes = own_ref[pl.ds(part, 1), :], size_ref[pl.ds(part, 1), :]
        tiles = range(0, rows, LOW)
        own_at = jnp.concatenate([column(places[:, t : t + LOW]) for t in tiles], 0).astype(jnp.int32)
        size = jnp.concatenate([column(sizes[:, t : t + LOW]) for t in tiles], 0)
        own = rows_at(own_at, data_ref.at[:, :width])
        total = counted(copy, buffer_ref, part * SPLIT, data_ref.at[:, width:])
        start = pl.multiple_of(part * rows, rows)
        out_ref[pl.ds(start, rows), :] = (own + total / size).astype(BF16)


def seeds(counts, places, sizes, first, second, own, near, far):
    targets, each = counts[0].shape
    width = second.shape[1] // 2
    parts, rows = places.shape
    return pl.pallas_call(
        seed_kernel,
        in_specs=in_place(SPLIT) + in_vmem(6 + len(far)),
        out_specs=in_vmem(1)[0],
        out_shape=jax.ShapeDtypeStruct((targets, width), BF16),
        scratch_shapes=[
            pltpu.VMEM((SPLIT * each, 2 * width), BF16),
            pltpu.VMEM((parts * SPLIT, rows, each), BF16),
            *[pltpu.VMEM((own.shape[0], first.shape[1] // 2), BF16)] * 2,
            pltpu.SemaphoreType.DMA((parts * SPLIT,)),
        ],
        compiler_params=pltpu.CompilerParams(vmem_limit_bytes=30 * MIB),
        cost_estimate=pl.CostEstimate(
            flops=4 * targets * SPLIT * each * width,
            transcendentals=0,
            bytes_accessed=targets * SPLIT * each * 2,
        ),
        name="seeds",
    )(*[to_hbm(c) for c in counts], places, sizes, first, second, own, near, *far)


def shards(
    store_feat,
    want_in,
    nbr_in,
    self_in,
    count_in,
    weight_one,
    want_hid,
    nbr_hid,
    self_hid,
    count_hid,
    weight_two,
):
    x = lax.axis_index("wt") * 2 + lax.axis_index("xlo")
    core = lax.axis_index("core")
    parts = want_in.shape[1]
    block = want_in.shape[2] // CHIPS

    def mine(wanted):
        return lax.dynamic_slice_in_dim(wanted[0], block * x, block, 1).reshape(-1)

    def exchange(rows):
        pieces = rows.reshape(parts, block, rows.shape[1])
        return lax.all_to_all(pieces, "dom", 0, 0, tiled=True).reshape(rows.shape)

    together = lax.optimization_barrier
    positions = parts * block * CHIPS

    at = jnp.stack([x, core]).astype(jnp.int32)
    fetched = exchange(pick(want_in[0], at, store_feat, parts * block))

    table = node_table(nbr_in.T, self_in[None], count_in[None])
    requests = mine(want_hid)
    nodes, *counts, token = node_counts(requests, x, table, positions)
    fetched, token = together((fetched, token))
    below, above = send(fetched, UP), send(fetched, DOWN)
    code = codes(nbr_hid, count_hid, x)
    below, above, code = together((below, above, code))
    cut = below.shape[0] // 2
    far_low, far_high = send(below[:cut], UP), send(above[cut:], DOWN)
    *counts_two, token_two = slot_counts(code, positions, 0)
    weight_one, token_two = together((weight_one, token_two))
    first_blocks = [weight_one] + [send(weight_one, pairs) for pairs in (DOWN, ACROSS, UP)]
    pieces = (fetched, above, far_low, far_high, below)
    ready = own_and_mean(x, counts, nodes, pieces, (token, token_two))

    ready, weight_two, code, *first_blocks = together((ready, weight_two, code, *first_blocks))
    arrived = exchange(ready)
    other_rows = send(weight_two, ACROSS)
    *counts_two, token = slot_counts(code, positions, 1, counts_two)
    first_blocks = [b for block in first_blocks for b in (block, to_hbm(swap(block)))]
    own_at = place(self_hid, x).reshape(2, -1)
    sizes = count_hid.reshape(2, -1)
    arrived, own_at, sizes, token, weight_two, other_rows, *first_blocks = together(
        (arrived, own_at, sizes, token, weight_two, other_rows, *first_blocks)
    )
    first, second, ready = assemble(at, first_blocks, weight_two, other_rows)
    cut = arrived.shape[0] // 2
    low, high = arrived[:cut], arrived[cut:]
    below_low, above_high = send(low, UP), send(high, DOWN)
    below_high, above_low = send(high, UP), send(low, DOWN)
    other = swap(arrived)
    below_low, above_high, other, ready = together((below_low, above_high, other, ready))
    far_low = send(below_low, UP)
    far_high = send(above_high, DOWN)
    own = project(first, second, arrived, other, after=(token, ready))
    below_high, above_low, own = together((below_high, above_low, own))
    near = []
    for piece in (above_low, above_high, below_low, below_high):
        near += [piece, swap(piece)]
    near = project(first, second, *near)
    far_low, far_high, near = together((far_low, far_high, near))
    far = (far_low, swap(far_low), far_high, swap(far_high))
    return seeds(counts_two, own_at, sizes, first, second, own, near, far)


def solution(mesh):
    mesh = Mesh(mesh.devices.reshape(32, 2, 2, 2), ("dom", "xlo", "core", "wt"))
    columns = ("xlo", "core")
    return jax.shard_map(
        shards,
        mesh=mesh,
        in_specs=(
            P("dom", None),
            P("dom", None, None),
            P("dom", None),
            P("dom"),
            P("dom"),
            P("wt", columns),
            P("dom", None, None),
            P("dom", None),
            P("dom"),
            P("dom"),
            P("wt", columns),
        ),
        out_specs=P("dom", columns),
        check_vma=False,
    )
```

```python
import functools

import jax
import jax.numpy as jnp
from jax import lax
from jax.experimental import pallas as pl
from jax.experimental.pallas import tpu as pltpu
from jax.sharding import Mesh, PartitionSpec as P


BF16 = jnp.bfloat16
F32 = jnp.float32
MIB = 1 << 20
CHIPS = 4
LINE = ("xlo", "wt")
SLOTS = 16
FAN = 10
TOKEN = pltpu.HBM((8, 128), jnp.int32)
SPLIT = 4
LOW = 256


def in_place(count):
    return [pl.BlockSpec(memory_space=pl.ANY)] * count


def to_hbm(array):
    return pltpu.with_memory_space_constraint(array, pltpu.HBM)


def in_vmem(count):
    return [pl.BlockSpec(memory_space=pltpu.VMEM)] * count


def spot(x):
    return (x % 2) * 2 + x // 2


UP = [(spot(x), spot((x + 1) % CHIPS)) for x in range(CHIPS)]
DOWN = [(spot(x), spot((x - 1) % CHIPS)) for x in range(CHIPS)]
ACROSS = [(spot(x), spot((x + 2) % CHIPS)) for x in range(CHIPS)]
SWAP = [(0, 1), (1, 0)]


def send(block, pairs):
    return lax.ppermute(block, LINE, pairs)


def swap(block):
    return lax.ppermute(block, "core", SWAP)


def place(position, x):
    return ((((position >> 5) - x) & 3) << 10) | ((position >> 7) << 5) | (position & 31)


def write_counts(high, low, out_refs):
    slot = lax.broadcasted_iota(jnp.int32, (SLOTS, LOW), 0)
    lane = lax.broadcasted_iota(jnp.int32, (SLOTS, LOW), 1)
    expand = jnp.where((lane & (SLOTS - 1)) == slot, 1.0, 0.0).astype(BF16)
    high = dot(high.astype(F32).astype(BF16), expand)
    low = dot(low.astype(F32).astype(BF16), expand)
    target = lax.broadcasted_iota(jnp.int32, high.shape, 0)
    lane = lax.broadcasted_iota(jnp.int32, high.shape, 1)
    mine = (target & (SLOTS - 1)) == (lane >> 4)
    high = jnp.where(mine, high, -1.0).astype(BF16)
    low = jnp.where(mine, low, 0.0)
    rows = lax.broadcasted_iota(jnp.int32, (LOW, LOW), 0).astype(F32).astype(BF16)
    one = jnp.ones((), BF16)
    zero = jnp.zeros((), BF16)
    for g in range(high.shape[0] // SLOTS):
        mine_high = high[g * SLOTS : (g + 1) * SLOTS, :]
        left = jnp.concatenate(
            [jnp.where(mine_high == jnp.full((), k, BF16), one, zero) for k in range(SLOTS)], 0
        )
        mine_low = jnp.sum(low[g * SLOTS : (g + 1) * SLOTS, :], axis=0, keepdims=True).astype(BF16)
        right = jnp.where(rows == mine_low, one, zero)
        counts = lax.dot_general(left, right, (((1,), (1,)), ((), ())), preferred_element_type=F32)
        counts = counts.astype(BF16)
        store_counts(counts, out_refs, g * SLOTS)


def store_counts(counts, out_refs, start):
    each = SLOTS // SPLIT
    for k in range(SLOTS):
        out_refs[k // each][start : start + SLOTS, k % each * LOW : (k % each + 1) * LOW] = counts[
            k * SLOTS : (k + 1) * SLOTS, :
        ]


def own_and_total(index, counts_refs, self_ref, near_ref):
    rows = index.shape[0]
    lane = lax.broadcasted_iota(jnp.int32, (rows, LOW), 1).astype(F32).astype(BF16)
    spread = lambda a: jnp.broadcast_to(a.astype(F32), (rows, LOW)).astype(BF16)
    found = jnp.where(lane == spread(index & (LOW - 1)), spread(index >> 8), jnp.full((), -1, BF16))
    one, zero = jnp.ones((), BF16), jnp.zeros((), BF16)
    own, total, start = 0.0, 0.0, 0
    for ref in counts_refs:
        stop = start + ref.shape[1]
        hot = [
            jnp.where(found == jnp.full((), k, BF16), one, zero)
            for k in range(start // LOW, stop // LOW)
        ]
        own = own + dot(jnp.concatenate(hot, 1), self_ref[start:stop, :])
        total = total + dot(ref[...], near_ref[start:stop, :])
        start = stop
    return own, total


def table_kernel(slots_ref, own_ref, size_ref, out_ref, lines_ref):
    lines_ref[...] = jnp.zeros(lines_ref.shape, jnp.int32)
    lanes = lines_ref.shape[1]
    width = slots_ref.shape[1]
    base = pl.program_id(0) * width
    for b in range(width // lanes):
        at = slice(b * lanes, (b + 1) * lanes)
        lines_ref[:FAN, :] = slots_ref[:, at]
        lines_ref[FAN : FAN + 1, :] = own_ref[:, at]
        lines_ref[FAN + 1 : FAN + 2, :] = size_ref[:, at]
        start = pl.multiple_of(base + b * lanes, lanes)
        out_ref[pl.ds(start, lanes), :] = lines_ref[...].T


def node_table(slots, own, sizes):
    stored = slots.shape[1]
    step = 1024
    return pl.pallas_call(
        table_kernel,
        grid=(stored // step,),
        in_specs=[pl.BlockSpec((a.shape[0], step), lambda i: (0, i)) for a in (slots, own, sizes)],
        out_specs=in_vmem(1)[0],
        out_shape=jax.ShapeDtypeStruct((stored, SLOTS), jnp.int32),
        scratch_shapes=[pltpu.VMEM((SLOTS, 128), jnp.int32)],
        compiler_params=pltpu.CompilerParams(vmem_limit_bytes=2 * MIB),
        name="node_table",
    )(slots, own, sizes)


def node_kernel(request_ref, x_ref, table_ref, nodes_ref, *refs):
    out_refs, rows_ref = refs[:SPLIT], refs[-1]
    step = rows_ref.shape[0]
    base = pl.multiple_of(pl.program_id(0) * step, step)
    for i in range(step):
        rows_ref[i : i + 1, :] = table_ref[pl.ds(request_ref[base + i], 1), :]
    rows = rows_ref[...]
    nodes_ref[...] = rows
    size = rows[:, FAN + 1 : FAN + 2]
    at = place(rows, x_ref[0])
    valid = lax.broadcasted_iota(jnp.int32, rows.shape, 1) < size
    high = jnp.where(valid, at >> 8, -1)
    write_counts(high, at & (LOW - 1), out_refs)


def node_counts(requests, x, table, positions):
    targets = requests.shape[0]
    step = 256
    return pl.pallas_call(
        node_kernel,
        grid_spec=pltpu.PrefetchScalarGridSpec(
            num_scalar_prefetch=2,
            grid=(targets // step,),
            in_specs=in_vmem(1),
            out_specs=(
                *[pl.BlockSpec((step, SLOTS), lambda i, r, x: (i, 0))],
                *[pl.BlockSpec((step, positions // SPLIT), lambda i, r, x: (i, 0))] * SPLIT,
                *in_place(1),
            ),
            scratch_shapes=[pltpu.VMEM((step, SLOTS), jnp.int32)],
        ),
        out_shape=(
            pltpu.HBM((targets, SLOTS), jnp.int32),
            *[pltpu.HBM((targets, positions // SPLIT), BF16)] * SPLIT,
            TOKEN,
        ),
        compiler_params=pltpu.CompilerParams(vmem_limit_bytes=10 * MIB),
        cost_estimate=pl.CostEstimate(
            flops=targets * 2 * SLOTS * LOW * LOW, transcendentals=0, bytes_accessed=targets * positions * 2
        ),
        name="node_counts",
    )(requests, x.reshape(1), table)


def codes(neighbours, counts, x):
    targets, fan = neighbours.shape
    at = place(jnp.pad(neighbours, ((0, 0), (0, SLOTS - fan))), x)
    valid = lax.broadcasted_iota(jnp.int32, at.shape, 1) < counts[:, None]
    target = lax.broadcasted_iota(jnp.int32, at.shape, 0) & (SLOTS - 1)
    high = jnp.where(valid, (at >> 8) * SLOTS + target + 1, 0)
    return (high * LOW + (at & (LOW - 1))).reshape(targets // SLOTS, SLOTS * SLOTS)


def slot_kernel(code_ref, *refs):
    out_refs = refs[-SPLIT - 1 : -1]
    rows = lax.broadcasted_iota(jnp.int32, (LOW, LOW), 0).astype(F32).astype(BF16)
    one = jnp.ones((), BF16)
    zero = jnp.zeros((), BF16)
    code = code_ref[...]
    high = ((code >> 8) - 1).astype(F32)
    low = (code & (LOW - 1)).astype(F32)
    for g in range(code_ref.shape[0]):
        left = jnp.where(rows == high[g : g + 1, :].astype(BF16), one, zero)
        right = jnp.where(rows == low[g : g + 1, :].astype(BF16), one, zero)
        counts = lax.dot_general(left, right, (((1,), (1,)), ((), ())), preferred_element_type=F32)
        store_counts(counts.astype(BF16), out_refs, g * SLOTS)


def slot_counts(code, positions, part, before=()):
    groups, width = code.shape
    step = 16
    steps = groups // step // 2
    width_out = positions // SPLIT
    return pl.pallas_call(
        slot_kernel,
        grid=(steps,),
        in_specs=[pl.BlockSpec((step, width), lambda i: (i + part * steps, 0))]
        + in_place(len(before)),
        out_specs=(
            *[pl.BlockSpec((step * SLOTS, width_out), lambda i: (i + part * steps, 0))] * SPLIT,
            *in_place(1),
        ),
        out_shape=(*[pltpu.HBM((groups * SLOTS, width_out), BF16)] * SPLIT, TOKEN),
        input_output_aliases={i + 1: i for i in range(len(before))},
        compiler_params=pltpu.CompilerParams(vmem_limit_bytes=10 * MIB),
        cost_estimate=pl.CostEstimate(
            flops=groups * LOW * LOW * LOW,
            transcendentals=0,
            bytes_accessed=groups // 2 * SLOTS * positions * 2,
        ),
        name="slot_counts",
    )(code, *before)


def weight_kernel(at_ref, *refs):
    blocks, (mine_ref, other_ref, first_ref, second_ref, token_ref) = refs[:-5], refs[-5:]
    x, core = at_ref[0], at_ref[1]
    half = first_ref.shape[1] // 4
    for i, block in enumerate(blocks):
        chip = (x + i // 2) & (CHIPS - 1)
        column = 2 * (chip & 1) + (core if i % 2 == 0 else 1 - core)
        for side in range(2):
            start = pl.multiple_of(half * (core if side == 0 else 1 - core), half)
            at = pl.multiple_of((2 * side + (chip >> 1)) * half, half)
            first_ref[column, pl.ds(at, half), :] = block[pl.ds(start, half), :]
    columns = mine_ref.shape[1]

    @pl.when(x < 2)
    def _():
        second_ref[:, :columns] = mine_ref[...]
        second_ref[:, columns:] = other_ref[...]

    @pl.when(x >= 2)
    def _():
        second_ref[:, :columns] = other_ref[...]
        second_ref[:, columns:] = mine_ref[...]


def assemble(at, blocks, mine, other):
    k, width = blocks[0].shape
    first = (CHIPS, 2 * k, width)
    second = (mine.shape[0], 2 * mine.shape[1])
    return pl.pallas_call(
        weight_kernel,
        grid_spec=pltpu.PrefetchScalarGridSpec(
            num_scalar_prefetch=1,
            grid=(1,),
            in_specs=[
                pl.BlockSpec(b.shape, lambda i, at: (0, 0), pipeline_mode=pl.Buffered(1))
                for b in (*blocks, mine, other)
            ],
            out_specs=(*in_vmem(2), *in_place(1)),
        ),
        out_shape=(jax.ShapeDtypeStruct(first, BF16), jax.ShapeDtypeStruct(second, BF16), TOKEN),
        compiler_params=pltpu.CompilerParams(vmem_limit_bytes=10 * MIB),
        name="assemble",
    )(at, *[to_hbm(b) for b in (*blocks, mine, other)])


def column(row):
    shape = (row.shape[1], row.shape[1])
    diagonal = lax.broadcasted_iota(jnp.int32, shape, 0) == lax.broadcasted_iota(jnp.int32, shape, 1)
    return jnp.sum(jnp.where(diagonal, row.astype(F32), 0.0), axis=1, keepdims=True)


def dot(a, b):
    return jnp.dot(a, b, preferred_element_type=F32)


def load_rows(out_ref, data_ref, positions):
    for i, at in enumerate(positions):
        out_ref[i : i + 1, :] = data_ref[pl.ds(at, 1), :]


def pick_kernel(want_ref, at_ref, *refs):
    blocks, (out_ref, wide_ref, rows_ref) = refs[:-3], refs[-3:]
    start = 0
    for block in blocks:
        wide_ref[start : start + block.shape[0], :] = block[...].astype(F32)
        start += block.shape[0]
    parts = want_ref.shape[0]
    block = out_ref.shape[0] // parts
    base = at_ref[0] * block

    @pl.loop(0, parts)
    def _(p):
        load_rows(rows_ref, wide_ref, [want_ref[p, base + i] for i in range(block)])
        out_ref[pl.ds(pl.multiple_of(p * block, block), block), :] = rows_ref[...].astype(BF16)


def pick(want, at, stored, targets):
    rows, width = stored.shape[0] // SPLIT, stored.shape[1] // 2
    block = targets // want.shape[0]
    return pl.pallas_call(
        pick_kernel,
        grid_spec=pltpu.PrefetchScalarGridSpec(
            num_scalar_prefetch=2,
            grid=(1,),
            in_specs=[
                pl.BlockSpec((rows, width), lambda i, w, at, k=k: (k, at[1])) for k in range(SPLIT)
            ],
            out_specs=pl.BlockSpec((targets, width), lambda i, w, at: (0, 0)),
            scratch_shapes=[
                pltpu.VMEM((stored.shape[0], width), F32),
                pltpu.VMEM((block, width), F32),
            ],
        ),
        out_shape=jax.ShapeDtypeStruct((targets, width), BF16),
        compiler_params=pltpu.CompilerParams(vmem_limit_bytes=8 * MIB),
        name="pick",
    )(want, at, *[to_hbm(stored)] * SPLIT)


def mean_kernel(tokens, x_ref, *refs):
    counts_refs, nodes_ref, refs = refs[:SPLIT], refs[SPLIT], refs[SPLIT + 1 :]
    pieces, (out_ref, data_ref) = refs[tokens:-2], refs[-2:]
    width = out_ref.shape[1] // 2

    @pl.when(pl.program_id(0) == 0)
    def _():
        start = 0
        for piece in pieces:
            data_ref[start : start + piece.shape[0], :] = piece[...]
            start += piece.shape[0]

    own_at = place(nodes_ref[:, FAN : FAN + 1], x_ref[0])
    size = nodes_ref[:, FAN + 1 : FAN + 2].astype(F32)
    own, total = own_and_total(own_at, counts_refs, data_ref, data_ref)
    out_ref[:, :width] = own.astype(BF16)
    out_ref[:, width:] = (total / size).astype(BF16)


def own_and_mean(x, counts, nodes, pieces, after):
    targets, positions = counts[0].shape[0], SPLIT * counts[0].shape[1]
    width = pieces[0].shape[1]
    tile = 256
    return pl.pallas_call(
        functools.partial(mean_kernel, len(after)),
        grid_spec=pltpu.PrefetchScalarGridSpec(
            num_scalar_prefetch=1,
            grid=(targets // tile,),
            in_specs=[pl.BlockSpec((tile, positions // SPLIT), lambda i, x: (i, 0))] * SPLIT
            + [pl.BlockSpec((tile, SLOTS), lambda i, x: (i, 0))]
            + in_place(len(after))
            + in_vmem(len(pieces)),
            out_specs=pl.BlockSpec((tile, 2 * width), lambda i, x: (i, 0)),
            scratch_shapes=[
                pltpu.VMEM((positions, width), BF16),
            ],
        ),
        out_shape=pltpu.HBM((targets, 2 * width), BF16),
        compiler_params=pltpu.CompilerParams(vmem_limit_bytes=14 * MIB),
        cost_estimate=pl.CostEstimate(
            flops=4 * targets * positions * width,
            transcendentals=0,
            bytes_accessed=targets * positions * 2,
        ),
        name="own_and_mean",
    )(x.reshape(1), *[to_hbm(c) for c in counts], to_hbm(nodes), *map(to_hbm, after), *pieces)


def project_into(out_ref, start, mine_ref, other_ref, first_ref, second_ref):
    rows, k = mine_ref.shape
    tile = min(rows, 512)
    for at in range(0, rows, tile):
        mine, other = mine_ref[at : at + tile, :], other_ref[at : at + tile, :]
        acc = jnp.zeros((tile, out_ref.shape[1]), F32)
        for h in range(first_ref.shape[0]):
            pre = dot(mine, first_ref[h, :k, :]) + dot(other, first_ref[h, k:, :])
            hidden = jnp.maximum(pre, 0.0).astype(BF16)
            width = hidden.shape[1]
            acc = acc + dot(hidden, second_ref[h * width : (h + 1) * width, :])
        out_ref[start + at : start + at + tile, :] = acc.astype(BF16)


def project_kernel(tokens, first_ref, second_ref, *refs):
    pieces, out_ref = refs[tokens:-1], refs[-1]
    start = 0
    for mine, other in zip(pieces[::2], pieces[1::2]):
        project_into(out_ref, start, mine, other, first_ref, second_ref)
        start += mine.shape[0]


def project(first, second, *pieces, after=()):
    rows = sum(p.shape[0] for p in pieces[::2])
    k, width = pieces[0].shape[1], second.shape[1]
    return pl.pallas_call(
        functools.partial(project_kernel, len(after)),
        in_specs=in_vmem(2) + in_place(len(after)) + in_vmem(len(pieces)),
        out_specs=in_vmem(1)[0],
        out_shape=jax.ShapeDtypeStruct((rows, width), BF16),
        compiler_params=pltpu.CompilerParams(vmem_limit_bytes=8 * MIB),
        cost_estimate=pl.CostEstimate(
            flops=2 * rows * second.shape[0] * (2 * k + width),
            transcendentals=0,
            bytes_accessed=rows * (2 * k + width) * 2,
        ),
        name="project",
    )(first, second, *map(to_hbm, after), *pieces)


def seed_kernel(*refs):
    counts_refs, (own_ref, size_ref, first_ref, second_ref), refs = refs[:SPLIT], refs[SPLIT : SPLIT + 4], refs[SPLIT + 4 :]
    (mine_ref, near_ref), far, (out_ref, data_ref) = refs[:2], refs[2:-2], refs[-2:]
    width = out_ref.shape[1]
    block = mine_ref.shape[0]

    @pl.when(pl.program_id(0) == 0)
    def _():
        data_ref[:block, :] = mine_ref[...]
        data_ref[block : 2 * block, :] = near_ref[:block, :]
        data_ref[3 * block :, :] = near_ref[block:, :]
        start = 2 * block
        for mine, other in zip(far[::2], far[1::2]):
            project_into(data_ref, start, mine, other, first_ref, second_ref)
            start += mine.shape[0]

    own_at = column(own_ref[...]).astype(jnp.int32)
    own, total = own_and_total(own_at, counts_refs, data_ref.at[:, :width], data_ref.at[:, width:])
    out_ref[...] = (own + total / column(size_ref[...])).astype(BF16)


def seeds(places, counts, sizes, first, second, own, near, far):
    targets, positions = counts[0].shape[0], SPLIT * counts[0].shape[1]
    width = second.shape[1] // 2
    tile = 256
    return pl.pallas_call(
        seed_kernel,
        grid=(targets // tile,),
        in_specs=[pl.BlockSpec((tile, positions // SPLIT), lambda i: (i, 0))] * SPLIT
        + [pl.BlockSpec((1, tile), lambda i: (0, i))] * 2
        + in_vmem(4 + len(far)),
        out_specs=pl.BlockSpec((tile, width), lambda i: (i, 0)),
        out_shape=jax.ShapeDtypeStruct((targets, width), BF16),
        scratch_shapes=[pltpu.VMEM((positions, 2 * width), BF16)],
        compiler_params=pltpu.CompilerParams(vmem_limit_bytes=18 * MIB),
        cost_estimate=pl.CostEstimate(
            flops=4 * targets * positions * width,
            transcendentals=0,
            bytes_accessed=targets * positions * 2,
        ),
        name="seeds",
    )(*[to_hbm(c) for c in counts], places, sizes, first, second, own, near, *far)


def shards(
    store_feat,
    want_in,
    nbr_in,
    self_in,
    count_in,
    weight_one,
    want_hid,
    nbr_hid,
    self_hid,
    count_hid,
    weight_two,
):
    x = lax.axis_index("wt") * 2 + lax.axis_index("xlo")
    core = lax.axis_index("core")
    parts = want_in.shape[1]
    block = want_in.shape[2] // CHIPS

    def mine(wanted):
        return lax.dynamic_slice_in_dim(wanted[0], block * x, block, 1).reshape(-1)

    def exchange(rows):
        pieces = rows.reshape(parts, block, rows.shape[1])
        return lax.all_to_all(pieces, "dom", 0, 0, tiled=True).reshape(rows.shape)

    together = lax.optimization_barrier
    positions = parts * block * CHIPS

    at = jnp.stack([x, core]).astype(jnp.int32)
    fetched = exchange(pick(want_in[0], at, store_feat, parts * block))

    table = node_table(nbr_in.T, self_in[None], count_in[None])
    requests = mine(want_hid)
    nodes, *counts, token = node_counts(requests, x, table, positions)
    fetched, token = together((fetched, token))
    below, above = send(fetched, UP), send(fetched, DOWN)
    code = codes(nbr_hid, count_hid, x)
    below, above, code = together((below, above, code))
    cut = below.shape[0] // 2
    far_low, far_high = send(below[:cut], UP), send(above[cut:], DOWN)
    *counts_two, token_two = slot_counts(code, positions, 0)
    weight_one, token_two = together((weight_one, token_two))
    first_blocks = [weight_one] + [send(weight_one, pairs) for pairs in (DOWN, ACROSS, UP)]
    pieces = (fetched, above, far_low, far_high, below)
    ready = own_and_mean(x, counts, nodes, pieces, (token, token_two))

    ready, weight_two, code, *first_blocks = together((ready, weight_two, code, *first_blocks))
    arrived = exchange(ready)
    other_rows = send(weight_two, ACROSS)
    *counts_two, token = slot_counts(code, positions, 1, counts_two)
    first_blocks = [b for block in first_blocks for b in (block, to_hbm(swap(block)))]
    own_at = place(self_hid, x)[None]
    arrived, own_at, token, weight_two, other_rows, *first_blocks = together(
        (arrived, own_at, token, weight_two, other_rows, *first_blocks)
    )
    first, second, ready = assemble(at, first_blocks, weight_two, other_rows)
    cut = arrived.shape[0] // 2
    low, high = arrived[:cut], arrived[cut:]
    below_low, above_high = send(low, UP), send(high, DOWN)
    below_high, above_low = send(high, UP), send(low, DOWN)
    other = swap(arrived)
    below_low, above_high, other, ready = together((below_low, above_high, other, ready))
    far_low = send(below_low, UP)
    far_high = send(above_high, DOWN)
    own = project(first, second, arrived, other, after=(token, ready))
    below_high, above_low, own = together((below_high, above_low, own))
    near = []
    for piece in (above_low, above_high, below_low, below_high):
        near += [piece, swap(piece)]
    near = project(first, second, *near)
    far_low, far_high, near = together((far_low, far_high, near))
    far = (far_low, swap(far_low), far_high, swap(far_high))
    return seeds(own_at, counts_two, count_hid[None], first, second, own, near, far)


def solution(mesh):
    mesh = Mesh(mesh.devices.reshape(32, 2, 2, 2), ("dom", "xlo", "core", "wt"))
    columns = ("xlo", "core")
    return jax.shard_map(
        shards,
        mesh=mesh,
        in_specs=(
            P("dom", None),
            P("dom", None, None),
            P("dom", None),
            P("dom"),
            P("dom"),
            P("wt", columns),
            P("dom", None, None),
            P("dom", None),
            P("dom"),
            P("dom"),
            P("wt", columns),
        ),
        out_specs=P("dom", columns),
        check_vma=False,
    )
```
